32 devices in a mesh: dp: 8 (over z, y), mp: 4 (over x, core).
Axes of the slice: x: 2, y: 2, z: 4, core: 2. Of those that a mesh axis runs over, the one named last changes fastest.
Arguments:
- layer_input: bfloat16 [8, 1664, 512], P('dp'), may hold values from -6 to 6
- segments: int32 [8, 1664], P('dp'), may hold values from -1 to 12, as said below
- out_cotangent: bfloat16 [8, 1664, 512], P('dp'), may hold values from -6 to 6
- norm_gains: float32 [5, 512], replicated, may hold values from 0.5 to 1.5
- ffn1_in: bfloat16 [512, 2048], P(None, 'mp'), may hold values from -0.25 to 0.25
- ffn1_out: bfloat16 [2048, 512], P('mp'), may hold values from -0.125 to 0.125
- qkv_weight: bfloat16 [3, 512, 512], P(None, None, 'mp'), may hold values from -0.25 to 0.25
- pos_weight: bfloat16 [512, 512], P(None, 'mp'), may hold values from -0.25 to 0.25
- pos_bias: float32 [2, 512], P(None, 'mp'), may hold values from -3 to 3
- out_weight: bfloat16 [512, 512], P('mp'), may hold values from -2 to 2
- conv_in: bfloat16 [2, 512, 512], P(None, None, 'mp'), may hold values from -0.25 to 0.25
- depth_kernel: float32 [31, 512], P(None, 'mp'), may hold values from -1 to 1
- bn_scale: float32 [512], P('mp'), may hold values from 0.5 to 1.5
- bn_shift: float32 [512], P('mp'), may hold values from -3 to 3
- conv_out: bfloat16 [512, 512], P('mp'), may hold values from -0.25 to 0.25
- ffn2_in: bfloat16 [512, 2048], P(None, 'mp'), may hold values from -0.25 to 0.25
- ffn2_out: bfloat16 [2048, 512], P('mp'), may hold values from -0.125 to 0.125
Outputs:
- layer_output: bfloat16 [8, 1664, 512], P('dp')
- input_grad: bfloat16 [8, 1664, 512], P('dp')
- gains_grad: float32 [5, 512], P(None, 'dp')
- ffn1_in_grad: float32 [512, 2048], P('dp', 'mp')
- ffn1_out_grad: float32 [2048, 512], P('mp', 'dp')
- qkv_grad: float32 [3, 512, 512], P(None, 'dp', 'mp')
- pos_weight_grad: float32 [512, 512], P('dp', 'mp')
- pos_bias_grad: float32 [2, 512], P(None, 'mp')
- out_weight_grad: float32 [512, 512], P('mp', 'dp')
- conv_in_grad: float32 [2, 512, 512], P(None, 'dp', 'mp')
- kernel_grad: float32 [31, 512], P(None, 'mp')
- bn_scale_grad: float32 [512], P('mp')
- bn_shift_grad: float32 [512], P('mp')
- conv_out_grad: float32 [512, 512], P('mp', 'dp')
- ffn2_in_grad: float32 [512, 2048], P('dp', 'mp')
- ffn2_out_grad: float32 [2048, 512], P('mp', 'dp')
The draws below stay inside these ranges and needn't reach their ends.
Inputs may be any that keep to these rules, and one draw needn't show every extreme that they name: `segments`: within a row, utterances are numbered 0, 1, 2 in frame order, each a run of consecutive frames; the frames after a row's last utterance are -1. All utterances of one row come from one bucket: from 128 to 256 frames, from 320 to 640, or from 800 to 1600. The first row begins with an utterance of exactly 1600 frames; the second row is filled with utterances of exactly 128 frames.
All inputs are finite; a program needn't handle non-finite values.
Results may differ from the reference program's by a relative error of at most 0.025.
Values may be sent and summed in bfloat16 or wider, within the bound.
A program may use at most 320 MiB of HBM per device.

```python
import math
import jax
import jax.numpy as jnp
from jax import lax

D = 512
HEADS = 8
HEAD_DIM = 64
FF = 2048
KERNEL = 31
ROW_LEN = 1664
MAXLEN = 1600
ROWS = 8


def draw_segments(key, part):
    key_bucket, key_length = jax.random.split(jax.random.fold_in(key, 11))
    least = max(1, MAXLEN * 4 // 25 // 2)
    slots = ROW_LEN // least + 1
    bucket = jax.random.randint(key_bucket, (ROWS,), 0, 3)
    bucket = bucket.at[0].set(2)
    bucket = bucket.at[1].set(0)
    longest = jnp.where(bucket == 0, MAXLEN * 4 // 25, jnp.where(bucket == 1, MAXLEN * 2 // 5, MAXLEN))
    shortest = longest // 2
    raw_draw = jax.random.randint(key_length, (ROWS, slots), 0, 1 << 20)
    lengths = shortest[:, None] + raw_draw % (longest - shortest + 1)[:, None]
    lengths = lengths.at[0, 0].set(MAXLEN)
    lengths = lengths.at[1].set(jnp.full((slots,), least, jnp.int32))
    endings = jnp.cumsum(lengths, axis=1)
    places = jnp.arange(ROW_LEN)
    number = jnp.sum((endings[:, None, :] <= places[None, :, None]).astype(jnp.int32), axis=2)
    picks = jnp.arange(slots)
    end_here = jnp.sum(jnp.where(picks[None, None, :] == number[:, :, None], endings[:, None, :], 0), axis=2)
    inside = (number < slots) & (end_here <= ROW_LEN)
    return jnp.where(inside, number, -1).astype(jnp.int32)


def spiked(result, rng, source, target, parts, factor):
    owner, partner = [(jnp.arange(result.shape[axis_at]) // (result.shape[axis_at] // parts)).reshape([-1 if axis == axis_at else 1 for axis in range(result.ndim)]) for axis_at in (source, target)]
    chosen = jax.random.permutation(rng, parts)[partner]
    strong = (owner == chosen) | (owner == (partner + parts // 2) % parts)
    return jnp.where(strong, factor * result, result)


def level_of(key, dims, cuts, low, top_value):
    factor_of = 1.0
    for position, shards_of in cuts:
        heights = jax.random.uniform(jax.random.fold_in(jax.random.fold_in(key, 6), position), (shards_of,), jnp.float32, low / len(cuts), top_value / len(cuts))
        factor_of = factor_of * jnp.repeat(jnp.exp(heights), dims[position] // shards_of).reshape((-1,) + (1,) * (len(dims) - 1 - position))
    return factor_of


def bell_draw(rng, shape, deviation, bound, cuts=(), held_as=jnp.bfloat16):
    result = deviation * jax.random.normal(rng, shape, jnp.float32)
    if cuts:
        result = result * level_of(rng, shape, cuts, -0.22, 0.18)
    return jnp.clip(result, -bound, bound).astype(held_as)


def noise_with(rng, dims, width, most, cuts, heavy, kind=jnp.bfloat16):
    values = width * jax.random.normal(rng, dims, jnp.float32)
    if cuts:
        values = values * level_of(rng, dims, cuts, -0.22, 0.18)
    return jnp.clip(spiked(values, jax.random.fold_in(rng, 3), *heavy), -most, most).astype(kind)


def setup_inputs(seed: int = 0) -> dict:
    key_list = jax.random.split(jax.random.key(seed), 18)
    return {
        "layer_input": bell_draw(key_list[0], (ROWS, ROW_LEN, D), 1.0, 6.0, ((0, 8),)),
        "segments": draw_segments(jax.random.fold_in(key_list[17], 71), 0),
        "out_cotangent": noise_with(key_list[2], (ROWS, ROW_LEN, D), 1.0, 6.0, ((0, 8),), (0, 2, 8, 2.0)),
        "norm_gains": jnp.clip(1.0 + 0.1 * jax.random.normal(key_list[3], (5, D), jnp.float32), 0.5, 1.5),
        "ffn1_in": bell_draw(key_list[4], (D, FF), D ** -0.5, 0.25, ((1, 4),)),
        "ffn1_out": bell_draw(key_list[5], (FF, D), FF ** -0.5, 0.125, ((0, 4),)),
        "qkv_weight": bell_draw(key_list[6], (3, D, D), D ** -0.5, 0.25, ((2, 4),)),
        "pos_weight": bell_draw(key_list[7], (D, D), D ** -0.5, 0.25, ((1, 4),)),
        "pos_bias": bell_draw(key_list[8], (2, D), 0.5, 3.0, ((1, 4),), jnp.float32),
        "out_weight": bell_draw(key_list[9], (D, D), (D // 64) ** -0.5, 2.0, ((0, 4),)),
        "conv_in": bell_draw(key_list[10], (2, D, D), D ** -0.5, 0.25, ((2, 4),)),
        "depth_kernel": bell_draw(key_list[11], (KERNEL, D), KERNEL ** -0.5, 1.0, ((1, 4),), jnp.float32),
        "bn_scale": jnp.clip(1.0 + 0.1 * jax.random.normal(key_list[12], (D,), jnp.float32), 0.5, 1.5),
        "bn_shift": bell_draw(key_list[13], (D,), 0.5, 3.0, ((0, 4),), jnp.float32),
        "conv_out": bell_draw(key_list[14], (D, D), D ** -0.5, 0.25, ((0, 4),)),
        "ffn2_in": bell_draw(key_list[15], (D, FF), D ** -0.5, 0.25, ((1, 4),)),
        "ffn2_out": bell_draw(key_list[16], (FF, D), FF ** -0.5, 0.125, ((0, 4),)),
    }


NORM_EPSILON = 1e-05
HIGHEST_PRECISION = lax.Precision.HIGHEST

@jax.custom_vjp
def low(v):
    return lax.optimization_barrier(v.astype(jnp.bfloat16)).astype(jnp.float32)

@jax.custom_vjp
def low_back(v):
    return v

def low_keep(v):
    return (low(v), None)

def low_pass(kept, grad):
    return (grad,)

def back_keep(v):
    return (v, None)

def back_low(kept, grad):
    return (low(grad),)
low.defvjp(low_keep, low_pass)
low_back.defvjp(back_keep, back_low)

def highest_dot(first, second):
    return jnp.dot(first, second, precision=HIGHEST_PRECISION, preferred_element_type=jnp.float32)

def swish_value(value):
    return value * jax.nn.sigmoid(value)

def layer_norm(value, gain):
    centre = value - lax.optimization_barrier(jnp.mean(value, -1, keepdims=True))
    spread = lax.optimization_barrier(jnp.mean(centre * centre, -1, keepdims=True))
    return centre * lax.rsqrt(spread + NORM_EPSILON) * gain

def rel_table(frames, features):
    count_rows = 2 * frames - 1
    distance = (jnp.arange(count_rows) - (frames - 1)).astype(jnp.float32)
    freqs = jnp.exp(jnp.arange(features // 2).astype(jnp.float32) * (-2.0 * math.log(10000.0) / features))
    angles = distance[:, None] * freqs[None, :]
    return jnp.stack([jnp.sin(angles), jnp.cos(angles)], -1).reshape(count_rows, features)

def rel_shift(full):
    head_count, frames = (full.shape[0], full.shape[1])
    flat_rows = jnp.pad(full.reshape(head_count, frames * (2 * frames - 1)), ((0, 0), (0, frames)))
    return flat_rows.reshape(head_count, frames, 2 * frames)[:, :, :frames][:, :, ::-1]

def feed_forward(stream, gain, weight_in, weight_out):
    hidden = low(layer_norm(stream, gain))
    pre_act = low_back(highest_dot(hidden, weight_in))
    active = low(swish_value(pre_act))
    return low_back(highest_dot(active, weight_out))

def attend_row(row_u, row_v, row_keys, row_values, row_segment, pos_table):
    direct = jnp.einsum('ihd,jhd->hij', row_u, row_keys, precision=HIGHEST_PRECISION)
    shifted = rel_shift(jnp.einsum('ihd,chd->hic', row_v, pos_table, precision=HIGHEST_PRECISION))
    scores = low_back((direct + shifted) * HEAD_DIM ** (-0.5))
    matched = row_segment[:, None] == row_segment[None, :]
    scores = jnp.where(matched[None], scores, -1e+30)
    exponent = jnp.exp(scores - lax.optimization_barrier(jnp.max(scores, -1, keepdims=True)))
    probability = low(exponent / lax.optimization_barrier(jnp.sum(exponent, -1, keepdims=True)))
    return jnp.einsum('hij,jhd->ihd', probability, row_values, precision=HIGHEST_PRECISION)

def depthwise(channels, kernel, segments):
    margin = (KERNEL - 1) // 2
    padded = jnp.pad(channels, ((0, 0), (margin, margin), (0, 0)))
    seg_pad = jnp.pad(segments, ((0, 0), (margin, margin)), constant_values=-2)
    totals = jnp.zeros_like(channels)
    for offset in range(KERNEL):
        matched = (seg_pad[:, offset:offset + ROW_LEN] == segments).astype(jnp.float32)[..., None]
        totals = totals + kernel[offset] * padded[:, offset:offset + ROW_LEN] * matched
    return totals

def conformer(inputs, params, segments):
    gains, ffn1_in, ffn1_out, qkv_weight, pos_weight, pos_bias, out_weight, conv_in, depth_kernel, bn_scale, bn_shift, conv_out, ffn2_in, ffn2_out = params
    stream = inputs.reshape(-1, D)
    stream = stream + 0.5 * feed_forward(stream, gains[0], ffn1_in, ffn1_out)
    hidden = low(layer_norm(stream, gains[1]))
    queries = low_back(highest_dot(hidden, qkv_weight[0]))
    keys_low = low(low_back(highest_dot(hidden, qkv_weight[1])))
    values_low = low(low_back(highest_dot(hidden, qkv_weight[2])))
    q_u = low(queries + pos_bias[0])
    q_v = low(queries + pos_bias[1])
    pos_table = low(highest_dot(low(rel_table(ROW_LEN, D)), pos_weight)).reshape(2 * ROW_LEN - 1, HEADS, HEAD_DIM)
    shaped = (ROWS, ROW_LEN, HEADS, HEAD_DIM)
    checked = jax.checkpoint(attend_row)

    def one_row(pieces):
        return checked(pieces[0], pieces[1], pieces[2], pieces[3], pieces[4], pos_table)
    mixed = lax.map(one_row, (q_u.reshape(shaped), q_v.reshape(shaped), keys_low.reshape(shaped), values_low.reshape(shaped), segments))
    mixed = low(low_back(mixed.reshape(-1, D)))
    stream = stream + low_back(highest_dot(mixed, out_weight))
    hidden = low(layer_norm(stream, gains[2]))
    glu_value = low_back(highest_dot(hidden, conv_in[0]))
    glu_gate = low_back(highest_dot(hidden, conv_in[1]))
    channels = (glu_value * jax.nn.sigmoid(glu_gate)).reshape(ROWS, ROW_LEN, D)
    filtered = jax.checkpoint(depthwise)(channels, depth_kernel, segments)
    valid_mask = (segments >= 0).astype(jnp.float32)[..., None]
    frame_count = jnp.sum(valid_mask)
    bn_mean = lax.optimization_barrier(jnp.sum(valid_mask * filtered, (0, 1))) / frame_count
    centred = filtered - bn_mean
    bn_var = lax.optimization_barrier(jnp.sum(valid_mask * centred * centred, (0, 1))) / frame_count
    bn_value = centred * lax.rsqrt(bn_var + NORM_EPSILON) * bn_scale + bn_shift
    conv_act = low(swish_value(bn_value)).reshape(-1, D)
    stream = stream + low_back(highest_dot(conv_act, conv_out))
    stream = stream + 0.5 * feed_forward(stream, gains[3], ffn2_in, ffn2_out)
    return layer_norm(stream, gains[4]).reshape(ROWS, ROW_LEN, D)

def reference(layer_input, segments, out_cotangent, norm_gains, ffn1_in, ffn1_out, qkv_weight, pos_weight, pos_bias, out_weight, conv_in, depth_kernel, bn_scale, bn_shift, conv_out, ffn2_in, ffn2_out):
    params = (norm_gains, ffn1_in.astype(jnp.float32), ffn1_out.astype(jnp.float32), qkv_weight.astype(jnp.float32), pos_weight.astype(jnp.float32), pos_bias, out_weight.astype(jnp.float32), conv_in.astype(jnp.float32), depth_kernel, bn_scale, bn_shift, conv_out.astype(jnp.float32), ffn2_in.astype(jnp.float32), ffn2_out.astype(jnp.float32))

    def forward(inputs, *weights):
        return conformer(inputs, weights, segments)
    output, pullback = jax.vjp(forward, layer_input.astype(jnp.float32), *params)
    grads = pullback(out_cotangent.astype(jnp.float32))
    return (output.astype(jnp.bfloat16), grads[0].astype(jnp.bfloat16), grads[1], grads[2], grads[3], grads[4], grads[5], grads[6], grads[7], grads[8], grads[9], grads[10], grads[11], grads[12], grads[13], grads[14])
```

```python
import functools
import math

import jax
import jax.numpy as jnp
from jax import lax
from jax.experimental import pallas as pl
from jax.experimental.pallas import tpu as pltpu
from jax.sharding import PartitionSpec as P

HEAD_DIM = 64
BLOCK = 128
LANES = 128
NORM_EPSILON = 1e-05
SCALE = HEAD_DIM ** (-0.5)
F32 = jnp.float32
BF16 = jnp.bfloat16


def product(first, second):
    return jnp.dot(first, second, preferred_element_type=F32)


def left_product(first, second):
    return lax.dot_general(first, second, (((0,), (0,)), ((), ())), preferred_element_type=F32)


def right_product(first, second):
    return lax.dot_general(first, second, (((1,), (1,)), ((), ())), preferred_element_type=F32)


def swish_grad(value):
    sigmoid_out = jax.nn.sigmoid(value)
    return sigmoid_out * (1.0 + value * (1.0 - sigmoid_out))


def norm_forward(value):
    centre = value - jnp.mean(value, -1, keepdims=True)
    inverse = lax.rsqrt(jnp.mean(centre * centre, -1, keepdims=True) + NORM_EPSILON)
    return (centre * inverse, inverse)


def norm_backward(grad_out, normed, inverse, gain):
    scaled = grad_out * gain
    grad_in = inverse * (
        scaled
        - jnp.mean(scaled, -1, keepdims=True)
        - normed * jnp.mean(scaled * normed, -1, keepdims=True)
    )
    return (grad_in, jnp.sum(grad_out * normed, 0))


def bits_of(size):
    return [1 << step for step in range(size.bit_length() - 1)]


def swap(value, axis, bit):
    size = lax.axis_size(axis)
    return lax.ppermute(value, axis, [(rank, rank ^ bit) for rank in range(size)])


def pick(value, index, dim):
    return lax.dynamic_index_in_dim(value, index, dim, keepdims=False)


def gather_rows(share, axis):
    size, rank = lax.axis_size(axis), lax.axis_index(axis)
    held = {0: share}
    for bit in reversed(bits_of(size)):
        for offset, value in list(held.items()):
            held[offset ^ bit] = swap(value, axis, bit)
    rows = share.shape[0]
    whole = jnp.zeros((size * rows,) + share.shape[1:], share.dtype)
    for offset, value in held.items():
        start = (rank ^ offset) * rows
        whole = lax.dynamic_update_slice_in_dim(whole, value, start, 0)
    return whole


def scatter_chunks(chunks, axis):
    rank = lax.axis_index(axis)
    for bit in bits_of(lax.axis_size(axis)):
        count = chunks.shape[0] // 2
        pairs = chunks.reshape((count, 2) + chunks.shape[1:])
        mine = (rank // bit) % 2
        kept, sent = pick(pairs, mine, 1), pick(pairs, 1 - mine, 1)
        got = swap(sent.astype(BF16), axis, bit)
        chunks = kept.astype(F32) + got.astype(F32)
    return chunks[0]


def scatter_rows(value, axis):
    size = lax.axis_size(axis)
    return scatter_chunks(value.reshape((size, value.shape[0] // size) + value.shape[1:]), axis)


def sum_small(value, axis):
    for bit in bits_of(lax.axis_size(axis)):
        value = value + swap(value, axis, bit)
    return value


def merge_moments(count, mean, spread, axis):
    packed = jnp.concatenate([jnp.broadcast_to(count, mean.shape)[None], mean[None], spread[None]])
    for bit in bits_of(lax.axis_size(axis)):
        other = swap(packed, axis, bit)
        n_a, m_a, s_a = packed[0], packed[1], packed[2]
        n_b, m_b, s_b = other[0], other[1], other[2]
        total = n_a + n_b
        safe = jnp.maximum(total, 1.0)
        gap = m_a - m_b
        packed = jnp.stack(
            [
                total,
                (n_a * m_a + n_b * m_b) / safe,
                (s_a + s_b) + gap * gap * (n_a * n_b / safe),
            ]
        )
    return packed[0], packed[1], packed[2]


def trig_tables(frames, features):
    half = features // 2
    blocks = frames // BLOCK
    freqs = jnp.exp(jnp.arange(half).astype(F32) * (-2.0 * math.log(10000.0) / features))

    def both(places):
        angles = places.astype(F32)[:, None] * freqs[None, :]
        return jnp.sin(angles), jnp.cos(angles)

    s_a, c_a = both(jnp.arange(BLOCK // 16) * 16)
    s_b, c_b = both(jnp.arange(16))
    s_a, c_a, s_b, c_b = s_a[:, None], c_a[:, None], s_b[None], c_b[None]
    low_sin = (s_a * c_b + c_a * s_b).reshape(BLOCK, half)
    low_cos = (c_a * c_b - s_a * s_b).reshape(BLOCK, half)
    low = jnp.concatenate([low_sin, low_cos], 1)
    count = -(-blocks // 8) * 8
    s_h, c_h = both((jnp.arange(count) - blocks // 2) * BLOCK)
    high = jnp.concatenate([s_h, c_h], 1)
    high_t = jnp.pad(high, ((0, LANES - count), (0, 0))).T
    return low, high, low.T, high_t


def add_angles(s_h, c_h, s_l, c_l):
    return s_h * c_l + c_h * s_l, c_h * c_l - s_h * s_l


def head_rows(value, heads):
    owner = lax.broadcasted_iota(jnp.int32, value.shape, 0) // HEAD_DIM
    return jnp.concatenate([jnp.where(owner == h, value, 0.0) for h in range(heads)], 1)


def head_lanes(value, heads):
    owner = lax.broadcasted_iota(jnp.int32, value.shape, 1) // HEAD_DIM
    return jnp.concatenate([jnp.where(owner == h, value, 0.0) for h in range(heads)], 0)


def own_rows(value, heads):
    total = None
    for h in range(heads):
        piece = value[:, h * BLOCK : (h + 1) * BLOCK]
        owner = lax.broadcasted_iota(jnp.int32, piece.shape, 0) // HEAD_DIM
        piece = jnp.where(owner == h, piece, 0.0)
        total = piece if total is None else total + piece
    return total


def block_angles(low_t_ref, high_t_ref, block):
    half = low_t_ref.shape[0] // 2
    lane = lax.broadcasted_iota(jnp.int32, high_t_ref.shape, 1)
    column = jnp.sum(jnp.where(lane == block, high_t_ref[...], 0.0), 1, keepdims=True)
    return add_angles(column[:half], column[half:], low_t_ref[:half, :], low_t_ref[half:, :])


def fill_keys(key_ref, low_ref, high_ref, keys_s):
    features = low_ref.shape[1]
    half = features // 2
    width = key_ref.shape[1]
    keys_s[:, :width] = key_ref[...]
    for block in range(key_ref.shape[0] // BLOCK):
        rows = slice(block * BLOCK, (block + 1) * BLOCK)
        high = high_ref[block : block + 1, :]
        sine, cosine = add_angles(
            high[:, :half], high[:, half:], low_ref[:, :half], low_ref[:, half:]
        )
        keys_s[rows, width : width + half] = sine.astype(BF16)
        keys_s[rows, width + half :] = cosine.astype(BF16)


def fill_segments(seg_ref, seg_s):
    for block in range(seg_ref.shape[1] // BLOCK):
        rows = slice(block * BLOCK, (block + 1) * BLOCK)
        seg_s[rows, :] = jnp.broadcast_to(seg_ref[:, rows], (BLOCK, BLOCK)).T


def fill_queries(query_ref, bias_ref, table_ref, sine, cosine, heads, wide_s):
    query = query_ref[...]
    half = sine.shape[0]
    width = query.shape[1]
    q_u = (query + bias_ref[0:1, :]).astype(BF16).astype(F32)
    q_v = (query + bias_ref[1:2, :]).astype(BF16).astype(F32)
    wide_s[:width, :] = head_rows(q_u.T * SCALE, heads).astype(BF16)
    spread = head_rows(q_v.T * SCALE, heads).astype(BF16)
    for_sine = product(table_ref[:half, :], spread)
    for_cosine = product(table_ref[half:, :], spread)
    for h in range(heads):
        lanes = slice(h * BLOCK, (h + 1) * BLOCK)
        u_s, u_c = for_sine[:, lanes], for_cosine[:, lanes]
        wide_s[width : width + half, lanes] = (u_c * sine - u_s * cosine).astype(BF16)
        wide_s[width + half :, lanes] = (u_s * sine + u_c * cosine).astype(BF16)
    return q_u, q_v


def attend_kernel(
    heads,
    pieces,
    query_ref,
    key_ref,
    value_ref,
    seg_ref,
    seg_block_ref,
    bias_ref,
    table_ref,
    low_ref,
    high_ref,
    low_t_ref,
    high_t_ref,
    mixed_ref,
    total_ref,
    keys_s,
    value_t_s,
    seg_s,
    wide_s,
    score_s,
    prob_s,
):
    frames = key_ref.shape[0]
    step = pl.program_id(0)

    @pl.when(step == 0)
    def _():
        fill_keys(key_ref, low_ref, high_ref, keys_s)
        fill_segments(seg_ref, seg_s)
        for block in range(frames // BLOCK):
            rows = slice(block * BLOCK, (block + 1) * BLOCK)
            value_t_s[:, rows] = value_ref[rows, :].astype(F32).T.astype(BF16)

    sine, cosine = block_angles(low_t_ref, high_t_ref, step)
    fill_queries(query_ref, bias_ref, table_ref, sine, cosine, heads, wide_s)
    peaks = [None] * heads
    for rows in pieces:
        scores = product(keys_s[rows, :], wide_s[...])
        linked = seg_s[rows, :] == seg_block_ref[...]
        for h in range(heads):
            lanes = slice(h * BLOCK, (h + 1) * BLOCK)
            part = jnp.where(linked, scores[:, lanes], -1e30)
            score_s[rows, lanes] = part
            peak = jnp.max(part, 0, keepdims=True)
            peaks[h] = peak if peaks[h] is None else jnp.maximum(peaks[h], peak)
    sums = [None] * heads
    for rows in pieces:
        for h in range(heads):
            lanes = slice(h * BLOCK, (h + 1) * BLOCK)
            part = jnp.exp(score_s[rows, lanes] - peaks[h])
            prob_s[rows, lanes] = part.astype(BF16)
            extra = jnp.sum(part, 0, keepdims=True)
            sums[h] = extra if sums[h] is None else sums[h] + extra
    mixed = product(value_t_s[...], prob_s[...])
    mixed = mixed / jnp.concatenate(sums, 1)
    mixed_ref[...] = own_rows(mixed, heads).T.astype(BF16)
    for h in range(heads):
        total_ref[h : h + 1, :] = peaks[h] + jnp.log(sums[h])


def attend_back_kernel(
    heads,
    pieces,
    query_ref,
    key_ref,
    value_ref,
    grad_ref,
    mixed_ref,
    total_ref,
    seg_ref,
    seg_block_ref,
    bias_ref,
    table_ref,
    table_t_ref,
    low_ref,
    high_ref,
    low_t_ref,
    high_t_ref,
    query_g_ref,
    key_g_ref,
    value_g_ref,
    table_g_ref,
    bias_g_ref,
    keys_s,
    keys_t_s,
    seg_s,
    wide_s,
    wide_g_s,
    key_g_s,
    value_g_s,
):
    frames, width = key_ref.shape
    features = low_ref.shape[1]
    half = features // 2
    step = pl.program_id(0)

    @pl.when(step == 0)
    def _():
        fill_keys(key_ref, low_ref, high_ref, keys_s)
        fill_segments(seg_ref, seg_s)
        for block in range(frames // BLOCK):
            rows = slice(block * BLOCK, (block + 1) * BLOCK)
            keys_t_s[:width, rows] = key_ref[rows, :].astype(F32).T.astype(BF16)
            s_j, c_j = block_angles(low_t_ref, high_t_ref, block)
            keys_t_s[width : width + half, rows] = s_j.astype(BF16)
            keys_t_s[width + half :, rows] = c_j.astype(BF16)
        key_g_s[...] = jnp.zeros_like(key_g_s)
        value_g_s[...] = jnp.zeros_like(value_g_s)
        table_g_ref[...] = jnp.zeros_like(table_g_ref)
        bias_g_ref[...] = jnp.zeros_like(bias_g_ref)

    sine, cosine = block_angles(low_t_ref, high_t_ref, step)
    q_u, q_v = fill_queries(query_ref, bias_ref, table_ref, sine, cosine, heads, wide_s)
    grad = grad_ref[...].astype(F32)
    grad_t = grad.T
    weighted = (grad * mixed_ref[...].astype(F32)).T
    owner = lax.broadcasted_iota(jnp.int32, weighted.shape, 0) // HEAD_DIM
    slopes = [
        jnp.sum(jnp.where(owner == h, weighted, 0.0), 0, keepdims=True) for h in range(heads)
    ]
    grad_wide = head_rows(grad_t, heads).astype(BF16)
    grad_tall = head_lanes(grad, heads).astype(BF16)
    query_tall = head_lanes(q_u * SCALE, heads).astype(BF16)
    for number, rows in enumerate(pieces):
        scores = product(keys_s[rows, :], wide_s[...])
        prob_g = product(value_ref[rows, :], grad_wide)
        linked = seg_s[rows, :] == seg_block_ref[...]
        probs, score_gs = [], []
        for h in range(heads):
            lanes = slice(h * BLOCK, (h + 1) * BLOCK)
            part = jnp.where(linked, jnp.exp(scores[:, lanes] - total_ref[h : h + 1, :]), 0.0)
            probs.append(part.astype(BF16))
            score_gs.append((part * (prob_g[:, lanes] - slopes[h])).astype(BF16))
        prob = jnp.concatenate(probs, 1)
        score_g = jnp.concatenate(score_gs, 1)
        value_g_s[rows, :] += product(prob, grad_tall)
        key_g_s[rows, :] += product(score_g, query_tall)
        part = product(keys_t_s[:, rows], score_g)
        if number == 0:
            wide_g_s[...] = part
        else:
            wide_g_s[...] += part
    direct = own_rows(wide_g_s[:width, :], heads) * SCALE
    turned = []
    for h in range(heads):
        lanes = slice(h * BLOCK, (h + 1) * BLOCK)
        d_s = wide_g_s[width : width + half, lanes] * SCALE
        d_c = wide_g_s[width + half :, lanes] * SCALE
        turned.append(
            jnp.concatenate([sine * d_c - cosine * d_s, cosine * d_c + sine * d_s], 0).astype(BF16)
        )
    turned = jnp.concatenate(turned, 1)
    table_g_ref[...] += product(turned, head_lanes(q_v, heads).astype(BF16))
    shifted = own_rows(product(table_t_ref[...], turned), heads)
    query_g_ref[...] = (direct + shifted).T.astype(BF16)
    bias_g_ref[:width, :] += direct
    bias_g_ref[width:, :] += shifted

    @pl.when(step == pl.num_programs(0) - 1)
    def _():
        key_g_ref[...] = key_g_s[...].astype(BF16)
        value_g_ref[...] = value_g_s[...].astype(BF16)


def whole(shape):
    return pl.BlockSpec(shape, lambda i: (0,) * len(shape))


def by_rows(width):
    return pl.BlockSpec((BLOCK, width), lambda i: (i, 0))


def by_lanes(count):
    return pl.BlockSpec((count, BLOCK), lambda i: (0, i))


def cut(frames, sizes):
    pieces, start = [], 0
    for size in sizes:
        if start < frames:
            stop = min(start + size, frames)
            pieces.append(slice(start, stop))
            start = stop
    return pieces


def attend(heads, query, keys, values, segment, bias, table, tables):
    frames, width = keys.shape
    low, high, low_t, high_t = tables
    features = low.shape[1]
    lanes = heads * BLOCK
    pieces = cut(frames, [512, 512] + [640] * frames)
    flops = 2 * frames * frames * lanes // BLOCK * (width + features + width)
    return pl.pallas_call(
        functools.partial(attend_kernel, heads, pieces),
        grid=(frames // BLOCK,),
        in_specs=[
            by_rows(width),
            whole(keys.shape),
            whole(values.shape),
            whole(segment.shape),
            by_lanes(1),
            whole(bias.shape),
            whole(table.shape),
            whole(low.shape),
            whole(high.shape),
            whole(low_t.shape),
            whole(high_t.shape),
        ],
        out_specs=[by_rows(width), by_lanes(heads)],
        out_shape=[
            jax.ShapeDtypeStruct((frames, width), BF16),
            jax.ShapeDtypeStruct((heads, frames), F32),
        ],
        scratch_shapes=[
            pltpu.VMEM((frames, width + features), BF16),
            pltpu.VMEM((width, frames), BF16),
            pltpu.VMEM((frames, BLOCK), F32),
            pltpu.VMEM((width + features, lanes), BF16),
            pltpu.VMEM((frames, lanes), F32),
            pltpu.VMEM((frames, lanes), BF16),
        ],
        cost_estimate=pl.CostEstimate(
            flops=flops, bytes_accessed=8 * frames * width, transcendentals=frames * frames * heads
        ),
        name="attend",
    )(query, keys, values, segment, segment, bias, table, low, high, low_t, high_t)


def attend_back(heads, query, keys, values, grad, mixed, total, segment, bias, table, tables):
    frames, width = keys.shape
    low, high, low_t, high_t = tables
    features = low.shape[1]
    lanes = heads * BLOCK
    pieces = cut(frames, [512, 512] + [640] * frames)
    flops = 2 * frames * frames * lanes // BLOCK * (2 * (width + features) + 3 * width)
    return pl.pallas_call(
        functools.partial(attend_back_kernel, heads, pieces),
        grid=(frames // BLOCK,),
        in_specs=[
            by_rows(width),
            whole(keys.shape),
            whole(values.shape),
            by_rows(width),
            by_rows(width),
            by_lanes(heads),
            whole(segment.shape),
            by_lanes(1),
            whole(bias.shape),
            whole(table.shape),
            whole((width, features)),
            whole(low.shape),
            whole(high.shape),
            whole(low_t.shape),
            whole(high_t.shape),
        ],
        out_specs=[
            by_rows(width),
            whole(keys.shape),
            whole(values.shape),
            whole(table.shape),
            whole((2 * width, BLOCK)),
        ],
        out_shape=[
            jax.ShapeDtypeStruct((frames, width), BF16),
            jax.ShapeDtypeStruct(keys.shape, BF16),
            jax.ShapeDtypeStruct(values.shape, BF16),
            jax.ShapeDtypeStruct(table.shape, F32),
            jax.ShapeDtypeStruct((2 * width, BLOCK), F32),
        ],
        scratch_shapes=[
            pltpu.VMEM((frames, width + features), BF16),
            pltpu.VMEM((width + features, frames), BF16),
            pltpu.VMEM((frames, BLOCK), F32),
            pltpu.VMEM((width + features, lanes), BF16),
            pltpu.VMEM((width + features, lanes), F32),
            pltpu.VMEM((frames, width), F32),
            pltpu.VMEM((frames, width), F32),
        ],
        cost_estimate=pl.CostEstimate(
            flops=flops, bytes_accessed=16 * frames * width, transcendentals=frames * frames * heads
        ),
        name="attend_back",
    )(
        query,
        keys,
        values,
        grad,
        mixed,
        total,
        segment,
        segment,
        bias,
        table,
        table.T,
        low,
        high,
        low_t,
        high_t,
    )


def reach_of(segment, margin):
    frames = segment.shape[0]
    wide = jnp.pad(segment, (margin, margin), constant_values=-2)
    before = sum(
        (wide[margin - d : margin - d + frames] == segment).astype(F32)
        for d in range(1, margin + 1)
    )
    after = sum(
        (wide[margin + d : margin + d + frames] == segment).astype(F32)
        for d in range(1, margin + 1)
    )
    return before, after


EDGE = 16


def conv_kernel(taps, source_ref, weight_ref, before_ref, after_ref, out_ref, wide_s):
    frames, width = source_ref.shape
    margin = (taps - 1) // 2
    edge = jnp.zeros((EDGE, width), F32)
    wide_s[:EDGE, :] = edge
    wide_s[EDGE + frames :, :] = edge
    wide_s[EDGE : EDGE + frames, :] = source_ref[...]

    def one(block, carry):
        base = pl.multiple_of(block * BLOCK, BLOCK)
        before = before_ref[pl.ds(base, BLOCK), :]
        after = after_ref[pl.ds(base, BLOCK), :]
        total = source_ref[pl.ds(base, BLOCK), :] * weight_ref[margin : margin + 1, :]
        for d in range(1, margin + 1):
            prior = wide_s[pl.ds(base + (EDGE - d), BLOCK), :]
            later = wide_s[pl.ds(base + (EDGE + d), BLOCK), :]
            low, high = weight_ref[margin - d : margin - d + 1, :], weight_ref[margin + d : margin + d + 1, :]
            total = total + jnp.where(before >= d, prior, 0.0) * low
            total = total + jnp.where(after >= d, later, 0.0) * high
        out_ref[pl.ds(base, BLOCK), :] = total
        return carry

    lax.fori_loop(0, frames // BLOCK, one, 0)


def conv_back_kernel(
    taps, grad_ref, source_ref, weight_ref, before_ref, after_ref, out_ref, weight_g_ref, grad_s, source_s
):
    frames, width = source_ref.shape
    margin = (taps - 1) // 2
    edge = jnp.zeros((EDGE, width), F32)
    for wide_s, ref in ((grad_s, grad_ref), (source_s, source_ref)):
        wide_s[:EDGE, :] = edge
        wide_s[EDGE + frames :, :] = edge
        wide_s[EDGE : EDGE + frames, :] = ref[...]
    weight_g_ref[...] = jnp.zeros_like(weight_g_ref)

    def fold(value):
        return jnp.sum(value.reshape(BLOCK // 8, 8, width), 0)

    def one(block, carry):
        base = pl.multiple_of(block * BLOCK, BLOCK)
        before = before_ref[pl.ds(base, BLOCK), :]
        after = after_ref[pl.ds(base, BLOCK), :]
        grad = grad_ref[pl.ds(base, BLOCK), :]
        total = grad * weight_ref[margin : margin + 1, :]
        weight_g_ref[8 * margin : 8 * margin + 8, :] += fold(grad * source_ref[pl.ds(base, BLOCK), :])
        for d in range(1, margin + 1):
            for sign, reach in ((-1, before), (1, after)):
                near = margin + sign * d
                far = margin - sign * d
                open_ = reach >= d
                start = base + (EDGE + sign * d)
                total = total + jnp.where(open_, grad_s[pl.ds(start, BLOCK), :], 0.0) * weight_ref[far : far + 1, :]
                weight_g_ref[8 * near : 8 * near + 8, :] += fold(
                    jnp.where(open_, source_s[pl.ds(start, BLOCK), :], 0.0) * grad
                )
        out_ref[pl.ds(base, BLOCK), :] = total
        return carry

    lax.fori_loop(0, frames // BLOCK, one, 0)


def vmem_specs(count):
    return [pl.BlockSpec(memory_space=pltpu.VMEM)] * count


def depthwise(source, weight, before, after):
    frames, width = source.shape
    taps = weight.shape[0]
    return pl.pallas_call(
        functools.partial(conv_kernel, taps),
        in_specs=vmem_specs(4),
        out_specs=pl.BlockSpec(memory_space=pltpu.VMEM),
        out_shape=jax.ShapeDtypeStruct(source.shape, F32),
        scratch_shapes=[pltpu.VMEM((frames + 2 * EDGE, width), F32)],
        cost_estimate=pl.CostEstimate(
            flops=4 * taps * frames * width, bytes_accessed=16 * frames * width, transcendentals=0
        ),
        name="depthwise",
    )(source, weight, before, after)


def depthwise_back(grad, source, weight, before, after):
    frames, width = source.shape
    taps = weight.shape[0]
    out, sums = pl.pallas_call(
        functools.partial(conv_back_kernel, taps),
        in_specs=vmem_specs(5),
        out_specs=vmem_specs(2),
        out_shape=[
            jax.ShapeDtypeStruct(source.shape, F32),
            jax.ShapeDtypeStruct((8 * taps, width), F32),
        ],
        scratch_shapes=[pltpu.VMEM((frames + 2 * EDGE, width), F32)] * 2,
        cost_estimate=pl.CostEstimate(
            flops=8 * taps * frames * width, bytes_accessed=20 * frames * width, transcendentals=0
        ),
        name="depthwise_back",
    )(grad, source, weight, before, after)
    return out, jnp.sum(sums.reshape(taps, 8, width), 1)


def pad_lanes(value):
    width = value.shape[-1]
    extra = -width % LANES
    if not extra:
        return value
    return jnp.pad(value, [(0, 0)] * (value.ndim - 1) + [(0, extra)])


def swish_low(value):
    return (value * jax.nn.sigmoid(value)).astype(BF16)


def per_device(
    layer_input,
    segments,
    out_cotangent,
    norm_gains,
    ffn1_in,
    ffn1_out,
    qkv_weight,
    pos_weight,
    pos_bias,
    out_weight,
    conv_in,
    depth_kernel,
    bn_scale,
    bn_shift,
    conv_out,
    ffn2_in,
    ffn2_out,
):
    rows, frames, features = layer_input.shape
    assert rows == 1 and frames % BLOCK == 0
    segment = segments[0]
    model = lax.axis_size("mp")
    data = lax.axis_size("dp")
    share_rows = frames // model
    share_start = lax.axis_index("mp") * share_rows

    def take_share(value):
        return lax.dynamic_slice_in_dim(value, share_start, share_rows, 0)

    def spread(value):
        return gather_rows(value.astype(BF16), "mp")

    def reduce(value):
        return scatter_rows(value, "mp")

    def by_owner(grad):
        return grad.reshape(data, grad.shape[0] // data, grad.shape[1])

    flat_input = layer_input[0].astype(F32)
    flat_grad = out_cotangent[0].astype(F32)

    normed_all, _ = norm_forward(flat_input)
    hidden_1 = (normed_all * norm_gains[0]).astype(BF16)
    pre_1 = product(hidden_1, ffn1_in)
    active_1 = swish_low(pre_1)
    share_0 = take_share(flat_input)
    share = share_0 + 0.5 * reduce(product(active_1, ffn1_out))
    normed_1, inverse_1 = norm_forward(share_0)

    width = qkv_weight.shape[2]
    heads = width // HEAD_DIM
    tables = trig_tables(frames, features)
    table = jnp.concatenate([pos_weight[0::2], pos_weight[1::2]], 0)
    table_wide = pad_lanes(table)
    bias_wide = pad_lanes(pos_bias)
    segment_row = segment.astype(F32)[None]
    normed_2, inverse_2 = norm_forward(share)
    hidden_2 = spread(normed_2 * norm_gains[1])
    query = pad_lanes(product(hidden_2, qkv_weight[0]))
    keys = pad_lanes(product(hidden_2, qkv_weight[1]).astype(BF16))
    values = pad_lanes(product(hidden_2, qkv_weight[2]).astype(BF16))
    mixed_wide, totals = attend(
        heads, query, keys, values, segment_row, bias_wide, table_wide, tables
    )
    mixed = mixed_wide[:, :width]
    share = share + reduce(product(mixed, out_weight))

    normed_3, inverse_3 = norm_forward(share)
    hidden_3 = spread(normed_3 * norm_gains[2])
    glu_value = product(hidden_3, conv_in[0])
    gate_sig = jax.nn.sigmoid(product(hidden_3, conv_in[1]))
    channels = glu_value * gate_sig
    taps = depth_kernel.shape[0]
    before, after = reach_of(segment, (taps - 1) // 2)
    before = jnp.broadcast_to(before[:, None], channels.shape)
    after = jnp.broadcast_to(after[:, None], channels.shape)
    filtered = depthwise(channels, depth_kernel, before, after)
    valid = (segment >= 0).astype(F32)[:, None]
    count = jnp.sum(valid)
    mean = jnp.sum(valid * filtered, 0) / jnp.maximum(count, 1.0)
    off = filtered - mean
    spread_sum = jnp.sum(valid * off * off, 0)
    counts, bn_mean, bn_square = merge_moments(count, mean, spread_sum, "dp")
    bn_rstd = lax.rsqrt(bn_square / counts + NORM_EPSILON)
    centred = filtered - bn_mean
    bn_normed = centred * bn_rstd
    bn_value = bn_normed * bn_scale + bn_shift
    conv_act = swish_low(bn_value)
    share = share + reduce(product(conv_act, conv_out))

    normed_4, inverse_4 = norm_forward(share)
    hidden_4 = spread(normed_4 * norm_gains[3])
    pre_4 = product(hidden_4, ffn2_in)
    active_4 = swish_low(pre_4)
    share = share + 0.5 * reduce(product(active_4, ffn2_out))
    normed_5, inverse_5 = norm_forward(share)
    layer_output = spread(normed_5 * norm_gains[4])[None]

    gradient, gain_5 = norm_backward(take_share(flat_grad), normed_5, inverse_5, norm_gains[4])

    def ffn_back(gradient, gain, weight_in, weight_out, stored):
        normed, inverse, hidden, pre_act, active = stored
        grad_out = spread(0.5 * gradient)
        grad_pre = (right_product(grad_out, weight_out) * swish_grad(pre_act)).astype(BF16)
        grad_hidden = reduce(right_product(grad_pre, weight_in))
        grad_stream, gain_g = norm_backward(grad_hidden, normed, inverse, gain)
        in_g = scatter_chunks(by_owner(left_product(hidden, grad_pre).astype(BF16)), "dp")
        out_g = scatter_chunks(by_owner(left_product(grad_out, active).astype(BF16)), "dp").T
        return gradient + grad_stream, gain_g, in_g, out_g

    gradient, gain_4, ffn2_in_g, ffn2_out_g = ffn_back(
        gradient, norm_gains[3], ffn2_in, ffn2_out, (normed_4, inverse_4, hidden_4, pre_4, active_4)
    )

    grad_y = spread(gradient)
    conv_out_g = scatter_chunks(by_owner(left_product(grad_y, conv_act).astype(BF16)), "dp").T
    grad_bn = right_product(grad_y, conv_out) * swish_grad(bn_value)
    bn_sums = sum_small(jnp.stack([jnp.sum(grad_bn, 0), jnp.sum(grad_bn * bn_normed, 0)]), "dp")
    shift_g, scale_g = bn_sums[0], bn_sums[1]
    grad_mean = -bn_scale * shift_g * bn_rstd
    grad_var = -0.5 * bn_scale * scale_g * bn_rstd * bn_rstd
    grad_filtered = (
        bn_scale * grad_bn * bn_rstd + valid * (grad_mean + 2.0 * grad_var * centred) / counts
    )
    grad_channels, kernel_local = depthwise_back(
        grad_filtered, channels, depth_kernel, before, after
    )
    grad_value = (grad_channels * gate_sig).astype(BF16)
    grad_gate = (grad_channels * glu_value * gate_sig * (1.0 - gate_sig)).astype(BF16)
    grad_hidden = reduce(right_product(grad_value, conv_in[0]) + right_product(grad_gate, conv_in[1]))
    grad_stream, gain_3 = norm_backward(grad_hidden, normed_3, inverse_3, norm_gains[2])
    gradient = gradient + grad_stream
    conv_in_g = scatter_chunks(
        by_owner(left_product(hidden_3, jnp.concatenate([grad_value, grad_gate], 1)).astype(BF16)), "dp"
    )
    conv_in_g = jnp.stack(jnp.split(conv_in_g, 2, 1))

    grad_y = spread(gradient)
    out_weight_g = scatter_chunks(by_owner(left_product(grad_y, mixed).astype(BF16)), "dp").T
    grad_mixed = pad_lanes(right_product(grad_y, out_weight).astype(BF16))
    query_g, key_g, value_g, table_g, bias_g = attend_back(
        heads, query, keys, values, grad_mixed, mixed_wide, totals, segment_row, bias_wide, table_wide, tables
    )
    query_g, key_g, value_g = query_g[:, :width], key_g[:, :width], value_g[:, :width]
    grad_hidden = reduce(
        right_product(query_g, qkv_weight[0])
        + right_product(key_g, qkv_weight[1])
        + right_product(value_g, qkv_weight[2])
    )
    grad_stream, gain_2 = norm_backward(grad_hidden, normed_2, inverse_2, norm_gains[1])
    gradient = gradient + grad_stream
    qkv_g = scatter_chunks(
        by_owner(left_product(hidden_2, jnp.concatenate([query_g, key_g, value_g], 1)).astype(BF16)), "dp"
    )
    qkv_g = jnp.stack(jnp.split(qkv_g, 3, 1))
    half = features // 2
    table_g = table_g[:, :width]
    pos_weight_g = jnp.stack([table_g[:half], table_g[half:]], 1).reshape(features, width)
    pos_weight_g = scatter_chunks(by_owner(pos_weight_g.astype(BF16)), "dp")
    bias_g = jnp.sum(bias_g, 1).reshape(2, -1)[:, :width]

    gradient, gain_1, ffn1_in_g, ffn1_out_g = ffn_back(
        gradient, norm_gains[0], ffn1_in, ffn1_out, (normed_1, inverse_1, hidden_1, pre_1, active_1)
    )
    input_grad = spread(gradient)[None]

    gains = sum_small(sum_small(jnp.stack([gain_1, gain_2, gain_3, gain_4, gain_5]), "mp"), "dp")
    gain_width = features // data
    gains = lax.dynamic_slice_in_dim(gains, lax.axis_index("dp") * gain_width, gain_width, 1)
    late = sum_small(jnp.concatenate([bias_g, kernel_local], 0), "dp")
    return (
        layer_output,
        input_grad,
        gains,
        ffn1_in_g,
        ffn1_out_g,
        qkv_g,
        pos_weight_g,
        late[:2],
        out_weight_g,
        conv_in_g,
        late[2:],
        scale_g,
        shift_g,
        conv_out_g,
        ffn2_in_g,
        ffn2_out_g,
    )


def solution(mesh):
    placed = (
        P("dp", None, None),
        P("dp", None),
        P("dp", None, None),
        P(),
        P(None, "mp"),
        P("mp", None),
        P(None, None, "mp"),
        P(None, "mp"),
        P(None, "mp"),
        P("mp", None),
        P(None, None, "mp"),
        P(None, "mp"),
        P("mp"),
        P("mp"),
        P("mp", None),
        P(None, "mp"),
        P("mp", None),
    )
    return jax.shard_map(
        per_device,
        mesh=mesh,
        in_specs=placed,
        out_specs=(
            P("dp", None, None),
            P("dp", None, None),
            P(None, "dp"),
            P("dp", "mp"),
            P("mp", "dp"),
            P(None, "dp", "mp"),
            P("dp", "mp"),
            P(None, "mp"),
            P("mp", "dp"),
            P(None, "dp", "mp"),
            P(None, "mp"),
            P("mp"),
            P("mp"),
            P("mp", "dp"),
            P("dp", "mp"),
            P("mp", "dp"),
        ),
        check_vma=False,
    )
```

```python
import functools
import math

import jax
import jax.numpy as jnp
from jax import lax
from jax.experimental import pallas as pl
from jax.experimental.pallas import tpu as pltpu
from jax.sharding import PartitionSpec as P

HEAD_DIM = 64
BLOCK = 128
LANES = 128
NORM_EPSILON = 1e-05
SCALE = HEAD_DIM ** (-0.5)
F32 = jnp.float32
BF16 = jnp.bfloat16


def product(first, second):
    return jnp.dot(first, second, preferred_element_type=F32)


def left_product(first, second):
    return lax.dot_general(first, second, (((0,), (0,)), ((), ())), preferred_element_type=F32)


def right_product(first, second):
    return lax.dot_general(first, second, (((1,), (1,)), ((), ())), preferred_element_type=F32)


def swish_grad(value):
    sigmoid_out = jax.nn.sigmoid(value)
    return sigmoid_out * (1.0 + value * (1.0 - sigmoid_out))


def norm_forward(value):
    centre = value - jnp.mean(value, -1, keepdims=True)
    inverse = lax.rsqrt(jnp.mean(centre * centre, -1, keepdims=True) + NORM_EPSILON)
    return (centre * inverse, inverse)


def norm_backward(grad_out, normed, inverse, gain):
    scaled = grad_out * gain
    return inverse * (
        scaled
        - jnp.mean(scaled, -1, keepdims=True)
        - normed * jnp.mean(scaled * normed, -1, keepdims=True)
    )


def bits_of(size):
    return [1 << step for step in range(size.bit_length() - 1)]


def swap(value, axis, bit):
    size = lax.axis_size(axis)
    return lax.ppermute(value, axis, [(rank, rank ^ bit) for rank in range(size)])


def pick(value, index, dim):
    return lax.dynamic_index_in_dim(value, index, dim, keepdims=False)


def gather_offsets(share, axis):
    held = {0: share}
    for bit in reversed(bits_of(lax.axis_size(axis))):
        for offset, value in list(held.items()):
            held[offset ^ bit] = swap(value, axis, bit)
    return [held[offset] for offset in range(len(held))]


def gather_rows(share, axis):
    size, rank = lax.axis_size(axis), lax.axis_index(axis)
    rows = share.shape[0]
    whole = jnp.zeros((size * rows,) + share.shape[1:], share.dtype)
    for offset, value in enumerate(gather_offsets(share, axis)):
        whole = lax.dynamic_update_slice_in_dim(whole, value, (rank ^ offset) * rows, 0)
    return whole


def scatter_offsets(blocks, axis, kind=BF16):
    for bit in bits_of(lax.axis_size(axis)):
        pairs = blocks.reshape((blocks.shape[0] // 2, 2) + blocks.shape[1:])
        got = swap(pairs[:, 1].astype(kind), axis, bit)
        blocks = pairs[:, 0].astype(F32) + got.astype(F32)
    return blocks[0]


def scatter_chunks(chunks, axis):
    rank = lax.axis_index(axis)
    for bit in bits_of(lax.axis_size(axis)):
        count = chunks.shape[0] // 2
        pairs = chunks.reshape((count, 2) + chunks.shape[1:])
        mine = (rank // bit) % 2
        kept, sent = pick(pairs, mine, 1), pick(pairs, 1 - mine, 1)
        got = swap(sent.astype(BF16), axis, bit)
        chunks = kept.astype(F32) + got.astype(F32)
    return chunks[0]


def sum_small(value, axis):
    for bit in bits_of(lax.axis_size(axis)):
        value = value + swap(value, axis, bit)
    return value


def turn(value, bit, count):
    width = value.shape[-1] // count
    return jnp.concatenate(
        [value[..., (k ^ bit) * width : ((k ^ bit) + 1) * width] for k in range(count)], -1
    )


def everywhere(value, join):
    count = lax.axis_size("mp")
    for bit in bits_of(count):
        value = join(value, turn(swap(value, "mp", bit), bit, count))
    for bit in bits_of(lax.axis_size("dp")):
        value = join(value, swap(value, "dp", bit))
    return value


def join_moments(one, other):
    n_a, m_a, s_a = one[0], one[1], one[2]
    n_b, m_b, s_b = other[0], other[1], other[2]
    total = n_a + n_b
    safe = jnp.maximum(total, 1.0)
    gap = m_a - m_b
    return jnp.stack(
        [total, (n_a * m_a + n_b * m_b) / safe, (s_a + s_b) + gap * gap * (n_a * n_b / safe)]
    )


def trig_tables(frames, features):
    half = features // 2
    blocks = frames // BLOCK
    freqs = jnp.exp(jnp.arange(half).astype(F32) * (-2.0 * math.log(10000.0) / features))

    def both(places):
        angles = places.astype(F32)[:, None] * freqs[None, :]
        return jnp.sin(angles), jnp.cos(angles)

    s_a, c_a = both(jnp.arange(BLOCK // 16) * 16)
    s_b, c_b = both(jnp.arange(16))
    s_a, c_a, s_b, c_b = s_a[:, None], c_a[:, None], s_b[None], c_b[None]
    low_sin = (s_a * c_b + c_a * s_b).reshape(BLOCK, half)
    low_cos = (c_a * c_b - s_a * s_b).reshape(BLOCK, half)
    low = jnp.concatenate([low_sin, low_cos], 1)
    count = -(-blocks // 8) * 8
    s_h, c_h = both((jnp.arange(count) - blocks // 2) * BLOCK)
    high = jnp.concatenate([s_h, c_h], 1)
    high_t = jnp.pad(high, ((0, LANES - count), (0, 0))).T
    return low, high, low.T, high_t


def add_angles(s_h, c_h, s_l, c_l):
    return s_h * c_l + c_h * s_l, c_h * c_l - s_h * s_l


def head_rows(value, heads):
    owner = lax.broadcasted_iota(jnp.int32, value.shape, 0) // HEAD_DIM
    return jnp.concatenate([jnp.where(owner == h, value, 0.0) for h in range(heads)], 1)


def head_lanes(value, heads):
    owner = lax.broadcasted_iota(jnp.int32, value.shape, 1) // HEAD_DIM
    return jnp.concatenate([jnp.where(owner == h, value, 0.0) for h in range(heads)], 0)


def own_rows(value, heads):
    total = None
    for h in range(heads):
        piece = value[:, h * BLOCK : (h + 1) * BLOCK]
        owner = lax.broadcasted_iota(jnp.int32, piece.shape, 0) // HEAD_DIM
        piece = jnp.where(owner == h, piece, 0.0)
        total = piece if total is None else total + piece
    return total


def block_angles(low_t_ref, high_t_ref, block):
    half = low_t_ref.shape[0] // 2
    lane = lax.broadcasted_iota(jnp.int32, high_t_ref.shape, 1)
    column = jnp.sum(jnp.where(lane == block, high_t_ref[...], 0.0), 1, keepdims=True)
    return add_angles(column[:half], column[half:], low_t_ref[:half, :], low_t_ref[half:, :])


def fill_keys(key_ref, low_ref, high_ref, keys_s):
    features = low_ref.shape[1]
    half = features // 2
    width = key_ref.shape[1]
    keys_s[:, :width] = key_ref[...]
    for block in range(key_ref.shape[0] // BLOCK):
        rows = slice(block * BLOCK, (block + 1) * BLOCK)
        high = high_ref[block : block + 1, :]
        sine, cosine = add_angles(
            high[:, :half], high[:, half:], low_ref[:, :half], low_ref[:, half:]
        )
        keys_s[rows, width : width + half] = sine.astype(BF16)
        keys_s[rows, width + half :] = cosine.astype(BF16)


def fill_segments(seg_ref, seg_s):
    for block in range(seg_ref.shape[1] // BLOCK):
        rows = slice(block * BLOCK, (block + 1) * BLOCK)
        seg_s[rows, :] = jnp.broadcast_to(seg_ref[:, rows], (BLOCK, BLOCK)).T


def fill_queries(query_ref, bias_ref, table_ref, sine, cosine, heads, wide_s):
    query = query_ref[...]
    half = sine.shape[0]
    width = query.shape[1]
    q_u = (query + bias_ref[0:1, :]).astype(BF16).astype(F32)
    q_v = (query + bias_ref[1:2, :]).astype(BF16).astype(F32)
    wide_s[:width, :] = head_rows(q_u.T * SCALE, heads).astype(BF16)
    spread = head_rows(q_v.T * SCALE, heads).astype(BF16)
    for_sine = product(table_ref[:half, :], spread)
    for_cosine = product(table_ref[half:, :], spread)
    for h in range(heads):
        lanes = slice(h * BLOCK, (h + 1) * BLOCK)
        u_s, u_c = for_sine[:, lanes], for_cosine[:, lanes]
        wide_s[width : width + half, lanes] = (u_c * sine - u_s * cosine).astype(BF16)
        wide_s[width + half :, lanes] = (u_s * sine + u_c * cosine).astype(BF16)
    return q_u, q_v


def attend_kernel(
    heads,
    pieces,
    query_ref,
    key_ref,
    value_ref,
    seg_ref,
    seg_block_ref,
    bias_ref,
    table_ref,
    low_ref,
    high_ref,
    low_t_ref,
    high_t_ref,
    mixed_ref,
    total_ref,
    keys_s,
    value_t_s,
    seg_s,
    wide_s,
    score_s,
    prob_s,
):
    frames = key_ref.shape[0]
    step = pl.program_id(0)

    @pl.when(step == 0)
    def _():
        fill_keys(key_ref, low_ref, high_ref, keys_s)
        fill_segments(seg_ref, seg_s)
        for block in range(frames // BLOCK):
            rows = slice(block * BLOCK, (block + 1) * BLOCK)
            value_t_s[:, rows] = value_ref[rows, :].astype(F32).T.astype(BF16)

    sine, cosine = block_angles(low_t_ref, high_t_ref, step)
    fill_queries(query_ref, bias_ref, table_ref, sine, cosine, heads, wide_s)
    peaks = [None] * heads
    for rows in pieces:
        scores = product(keys_s[rows, :], wide_s[...])
        linked = seg_s[rows, :] == seg_block_ref[...]
        for h in range(heads):
            lanes = slice(h * BLOCK, (h + 1) * BLOCK)
            part = jnp.where(linked, scores[:, lanes], -1e30)
            score_s[rows, lanes] = part
            peak = jnp.max(part, 0, keepdims=True)
            peaks[h] = peak if peaks[h] is None else jnp.maximum(peaks[h], peak)
    sums = [None] * heads
    for rows in pieces:
        for h in range(heads):
            lanes = slice(h * BLOCK, (h + 1) * BLOCK)
            part = jnp.exp(score_s[rows, lanes] - peaks[h])
            prob_s[rows, lanes] = part.astype(BF16)
            extra = jnp.sum(part, 0, keepdims=True)
            sums[h] = extra if sums[h] is None else sums[h] + extra
    mixed = product(value_t_s[...], prob_s[...])
    mixed = mixed / jnp.concatenate(sums, 1)
    mixed_ref[...] = own_rows(mixed, heads).T.astype(BF16)
    for h in range(heads):
        total_ref[h : h + 1, :] = peaks[h] + jnp.log(sums[h])


def attend_back_kernel(
    heads,
    pieces,
    query_ref,
    key_ref,
    value_ref,
    grad_ref,
    mixed_ref,
    total_ref,
    seg_ref,
    seg_block_ref,
    bias_ref,
    table_ref,
    table_t_ref,
    low_ref,
    high_ref,
    low_t_ref,
    high_t_ref,
    query_g_ref,
    key_g_ref,
    value_g_ref,
    table_g_ref,
    bias_g_ref,
    keys_s,
    keys_t_s,
    seg_s,
    wide_s,
    wide_g_s,
    key_g_s,
    value_g_s,
):
    frames, width = key_ref.shape
    features = low_ref.shape[1]
    half = features // 2
    step = pl.program_id(0)

    @pl.when(step == 0)
    def _():
        fill_keys(key_ref, low_ref, high_ref, keys_s)
        fill_segments(seg_ref, seg_s)
        for block in range(frames // BLOCK):
            rows = slice(block * BLOCK, (block + 1) * BLOCK)
            keys_t_s[:width, rows] = key_ref[rows, :].astype(F32).T.astype(BF16)
            s_j, c_j = block_angles(low_t_ref, high_t_ref, block)
            keys_t_s[width : width + half, rows] = s_j.astype(BF16)
            keys_t_s[width + half :, rows] = c_j.astype(BF16)
        key_g_s[...] = jnp.zeros_like(key_g_s)
        value_g_s[...] = jnp.zeros_like(value_g_s)
        table_g_ref[...] = jnp.zeros_like(table_g_ref)
        bias_g_ref[...] = jnp.zeros_like(bias_g_ref)

    sine, cosine = block_angles(low_t_ref, high_t_ref, step)
    q_u, q_v = fill_queries(query_ref, bias_ref, table_ref, sine, cosine, heads, wide_s)
    grad = grad_ref[...].astype(F32)
    grad_t = grad.T
    weighted = (grad * mixed_ref[...].astype(F32)).T
    owner = lax.broadcasted_iota(jnp.int32, weighted.shape, 0) // HEAD_DIM
    slopes = [
        jnp.sum(jnp.where(owner == h, weighted, 0.0), 0, keepdims=True) for h in range(heads)
    ]
    grad_wide = head_rows(grad_t, heads).astype(BF16)
    grad_tall = head_lanes(grad, heads).astype(BF16)
    query_tall = head_lanes(q_u * SCALE, heads).astype(BF16)
    for number, rows in enumerate(pieces):
        scores = product(keys_s[rows, :], wide_s[...])
        prob_g = product(value_ref[rows, :], grad_wide)
        linked = seg_s[rows, :] == seg_block_ref[...]
        probs, score_gs = [], []
        for h in range(heads):
            lanes = slice(h * BLOCK, (h + 1) * BLOCK)
            part = jnp.where(linked, jnp.exp(scores[:, lanes] - total_ref[h : h + 1, :]), 0.0)
            probs.append(part.astype(BF16))
            score_gs.append((part * (prob_g[:, lanes] - slopes[h])).astype(BF16))
        prob = jnp.concatenate(probs, 1)
        score_g = jnp.concatenate(score_gs, 1)
        value_g_s[rows, :] += product(prob, grad_tall)
        key_g_s[rows, :] += product(score_g, query_tall)
        part = product(keys_t_s[:, rows], score_g)
        if number == 0:
            wide_g_s[...] = part
        else:
            wide_g_s[...] += part
    direct = own_rows(wide_g_s[:width, :], heads) * SCALE
    turned = []
    for h in range(heads):
        lanes = slice(h * BLOCK, (h + 1) * BLOCK)
        d_s = wide_g_s[width : width + half, lanes] * SCALE
        d_c = wide_g_s[width + half :, lanes] * SCALE
        turned.append(
            jnp.concatenate([sine * d_c - cosine * d_s, cosine * d_c + sine * d_s], 0).astype(BF16)
        )
    turned = jnp.concatenate(turned, 1)
    table_g_ref[...] += product(turned, head_lanes(q_v, heads).astype(BF16))
    shifted = own_rows(product(table_t_ref[...], turned), heads)
    query_g_ref[...] = (direct + shifted).T.astype(BF16)
    bias_g_ref[:width, :] += direct
    bias_g_ref[width:, :] += shifted

    @pl.when(step == pl.num_programs(0) - 1)
    def _():
        key_g_ref[...] = key_g_s[...].astype(BF16)
        value_g_ref[...] = value_g_s[...].astype(BF16)


def whole(shape):
    return pl.BlockSpec(shape, lambda i: (0,) * len(shape))


def by_rows(width):
    return pl.BlockSpec((BLOCK, width), lambda i: (i, 0))


def by_lanes(count):
    return pl.BlockSpec((count, BLOCK), lambda i: (0, i))


def cut(frames, sizes):
    pieces, start = [], 0
    for size in sizes:
        if start < frames:
            stop = min(start + size, frames)
            pieces.append(slice(start, stop))
            start = stop
    return pieces


def attend(heads, query, keys, values, segment, bias, table, tables):
    frames, width = keys.shape
    low, high, low_t, high_t = tables
    features = low.shape[1]
    lanes = heads * BLOCK
    pieces = cut(frames, [512, 512] + [640] * frames)
    flops = 2 * frames * frames * lanes // BLOCK * (width + features + width)
    return pl.pallas_call(
        functools.partial(attend_kernel, heads, pieces),
        grid=(frames // BLOCK,),
        in_specs=[
            by_rows(width),
            whole(keys.shape),
            whole(values.shape),
            whole(segment.shape),
            by_lanes(1),
            whole(bias.shape),
            whole(table.shape),
            whole(low.shape),
            whole(high.shape),
            whole(low_t.shape),
            whole(high_t.shape),
        ],
        out_specs=[by_rows(width), by_lanes(heads)],
        out_shape=[
            jax.ShapeDtypeStruct((frames, width), BF16),
            jax.ShapeDtypeStruct((heads, frames), F32),
        ],
        scratch_shapes=[
            pltpu.VMEM((frames, width + features), BF16),
            pltpu.VMEM((width, frames), BF16),
            pltpu.VMEM((frames, BLOCK), F32),
            pltpu.VMEM((width + features, lanes), BF16),
            pltpu.VMEM((frames, lanes), F32),
            pltpu.VMEM((frames, lanes), BF16),
        ],
        cost_estimate=pl.CostEstimate(
            flops=flops, bytes_accessed=8 * frames * width, transcendentals=frames * frames * heads
        ),
        name="attend",
    )(query, keys, values, segment, segment, bias, table, low, high, low_t, high_t)


def attend_back(heads, query, keys, values, grad, mixed, total, segment, bias, table, tables):
    frames, width = keys.shape
    low, high, low_t, high_t = tables
    features = low.shape[1]
    lanes = heads * BLOCK
    pieces = cut(frames, [512, 512] + [640] * frames)
    flops = 2 * frames * frames * lanes // BLOCK * (2 * (width + features) + 3 * width)
    return pl.pallas_call(
        functools.partial(attend_back_kernel, heads, pieces),
        grid=(frames // BLOCK,),
        in_specs=[
            by_rows(width),
            whole(keys.shape),
            whole(values.shape),
            by_rows(width),
            by_rows(width),
            by_lanes(heads),
            whole(segment.shape),
            by_lanes(1),
            whole(bias.shape),
            whole(table.shape),
            whole((width, features)),
            whole(low.shape),
            whole(high.shape),
            whole(low_t.shape),
            whole(high_t.shape),
        ],
        out_specs=[
            by_rows(width),
            whole(keys.shape),
            whole(values.shape),
            whole(table.shape),
            whole((2 * width, BLOCK)),
        ],
        out_shape=[
            jax.ShapeDtypeStruct((frames, width), BF16),
            jax.ShapeDtypeStruct(keys.shape, BF16),
            jax.ShapeDtypeStruct(values.shape, BF16),
            jax.ShapeDtypeStruct(table.shape, F32),
            jax.ShapeDtypeStruct((2 * width, BLOCK), F32),
        ],
        scratch_shapes=[
            pltpu.VMEM((frames, width + features), BF16),
            pltpu.VMEM((width + features, frames), BF16),
            pltpu.VMEM((frames, BLOCK), F32),
            pltpu.VMEM((width + features, lanes), BF16),
            pltpu.VMEM((width + features, lanes), F32),
            pltpu.VMEM((frames, width), F32),
            pltpu.VMEM((frames, width), F32),
        ],
        cost_estimate=pl.CostEstimate(
            flops=flops, bytes_accessed=16 * frames * width, transcendentals=frames * frames * heads
        ),
        name="attend_back",
    )(
        query,
        keys,
        values,
        grad,
        mixed,
        total,
        segment,
        segment,
        bias,
        table,
        table.T,
        low,
        high,
        low_t,
        high_t,
    )


def reach_of(segment, margin):
    frames = segment.shape[0]
    wide = jnp.pad(segment, (margin, margin), constant_values=-2)
    before = sum(
        (wide[margin - d : margin - d + frames] == segment).astype(F32)
        for d in range(1, margin + 1)
    )
    after = sum(
        (wide[margin + d : margin + d + frames] == segment).astype(F32)
        for d in range(1, margin + 1)
    )
    return before, after


HALO = 16


def block_of(rows):
    return max(size for size in range(8, 65, 8) if rows % size == 0)


def lane_groups(width):
    size = min(width, LANES)
    return [slice(start, start + size) for start in range(0, width, size)]


def conv_kernel(taps, source_ref, weight_ref, before_ref, after_ref, out_ref, source_s):
    rows, width = out_ref.shape
    size = block_of(rows)
    margin = (taps - 1) // 2
    for group, lanes in enumerate(lane_groups(width)):
        source_s[group] = source_ref[:, lanes]

    def one(block, carry):
        base = pl.multiple_of(block * size, size)
        centre = pl.multiple_of(base + HALO, 8)
        for group, lanes in enumerate(lane_groups(width)):
            before = before_ref[pl.ds(centre, size), :]
            after = after_ref[pl.ds(centre, size), :]
            total = source_ref[pl.ds(centre, size), lanes] * weight_ref[margin : margin + 1, lanes]
            for d in range(1, margin + 1):
                for sign, reach in ((-1, before), (1, after)):
                    tap = margin + sign * d
                    other = source_s[group, pl.ds(base + (HALO + sign * d), size), :]
                    weight = weight_ref[tap : tap + 1, lanes]
                    total = total + jnp.where(reach >= d, other, 0.0) * weight
            out_ref[pl.ds(base, size), lanes] = total
        return carry

    lax.fori_loop(0, rows // size, one, 0)


def conv_back_kernel(
    taps, grad_ref, source_ref, weight_ref, before_ref, after_ref, out_ref, weight_g_ref, grad_s, source_s
):
    rows, width = out_ref.shape
    size = block_of(rows)
    margin = (taps - 1) // 2
    weight_g_ref[...] = jnp.zeros_like(weight_g_ref)
    for group, lanes in enumerate(lane_groups(width)):
        grad_s[group] = grad_ref[:, lanes]
        source_s[group] = source_ref[:, lanes]

    def fold(value):
        return jnp.sum(value.reshape(size // 8, 8, value.shape[1]), 0)

    def one(block, carry):
        base = pl.multiple_of(block * size, size)
        centre = pl.multiple_of(base + HALO, 8)
        middle = pl.multiple_of(base + 2 * HALO, 8)
        for group, lanes in enumerate(lane_groups(width)):
            before = before_ref[pl.ds(middle, size), :]
            after = after_ref[pl.ds(middle, size), :]
            grad = grad_ref[pl.ds(centre, size), lanes]
            total = grad * weight_ref[margin : margin + 1, lanes]
            weight_g_ref[8 * margin : 8 * margin + 8, lanes] += fold(
                grad * source_ref[pl.ds(middle, size), lanes]
            )
            for d in range(1, margin + 1):
                for sign, reach in ((-1, before), (1, after)):
                    near = margin + sign * d
                    far = margin - sign * d
                    linked = reach >= d
                    other = grad_s[group, pl.ds(base + (HALO + sign * d), size), :]
                    weight = weight_ref[far : far + 1, lanes]
                    total = total + jnp.where(linked, other, 0.0) * weight
                    other = source_s[group, pl.ds(base + (2 * HALO + sign * d), size), :]
                    weight_g_ref[8 * near : 8 * near + 8, lanes] += fold(
                        jnp.where(linked, other, 0.0) * grad
                    )
            out_ref[pl.ds(base, size), lanes] = total
        return carry

    lax.fori_loop(0, rows // size, one, 0)


def vmem_specs(count):
    return [pl.BlockSpec(memory_space=pltpu.VMEM)] * count


def grouped(rows, width):
    groups = lane_groups(width)
    return pltpu.VMEM((len(groups), rows, width // len(groups)), F32)


def depthwise(source, weight, before, after):
    rows, width = source.shape
    taps = weight.shape[0]
    return pl.pallas_call(
        functools.partial(conv_kernel, taps),
        in_specs=vmem_specs(4),
        out_specs=pl.BlockSpec(memory_space=pltpu.VMEM),
        out_shape=jax.ShapeDtypeStruct((rows - 2 * HALO, width), F32),
        scratch_shapes=[grouped(rows, width)],
        cost_estimate=pl.CostEstimate(
            flops=4 * taps * rows * width, bytes_accessed=16 * rows * width, transcendentals=0
        ),
        name="depthwise",
    )(source, weight, before, after)


def depthwise_back(grad, source, weight, before, after):
    rows, width = grad.shape
    taps = weight.shape[0]
    out, sums = pl.pallas_call(
        functools.partial(conv_back_kernel, taps),
        in_specs=vmem_specs(5),
        out_specs=vmem_specs(2),
        out_shape=[
            jax.ShapeDtypeStruct((rows - 2 * HALO, width), F32),
            jax.ShapeDtypeStruct((8 * taps, width), F32),
        ],
        scratch_shapes=[grouped(rows, width), grouped(rows + 2 * HALO, width)],
        cost_estimate=pl.CostEstimate(
            flops=8 * taps * rows * width, bytes_accessed=20 * rows * width, transcendentals=0
        ),
        name="depthwise_back",
    )(grad, source, weight, before, after)
    return out, jnp.sum(sums.reshape(taps, 8, width), 1)


def pad_lanes(value):
    width = value.shape[-1]
    extra = -width % LANES
    if not extra:
        return value
    return jnp.pad(value, [(0, 0)] * (value.ndim - 1) + [(0, extra)])


def swish_low(value):
    return (value * jax.nn.sigmoid(value)).astype(BF16)


def per_device(
    layer_input,
    segments,
    out_cotangent,
    norm_gains,
    ffn1_in,
    ffn1_out,
    qkv_weight,
    pos_weight,
    pos_bias,
    out_weight,
    conv_in,
    depth_kernel,
    bn_scale,
    bn_shift,
    conv_out,
    ffn2_in,
    ffn2_out,
):
    rows, frames, features = layer_input.shape
    assert rows == 1 and frames % BLOCK == 0
    segment = segments[0]
    model = lax.axis_size("mp")
    data = lax.axis_size("dp")
    share_rows = frames // model
    rank = lax.axis_index("mp")
    edge = 2 * HALO
    own = slice(HALO, HALO + share_rows)

    def piece(padded, owner):
        return lax.dynamic_slice_in_dim(padded, owner * share_rows, share_rows + 2 * edge, 0)

    def take(value, fill=0):
        pads = [(edge, edge)] + [(0, 0)] * (value.ndim - 1)
        return piece(jnp.pad(value, pads, constant_values=fill), rank)

    def reduce_wide(value):
        padded = jnp.pad(value.astype(BF16), ((edge, edge), (0, 0)))
        return scatter_offsets(jnp.stack([piece(padded, rank ^ k) for k in range(model)]), "mp")

    def reduce(value):
        value = value.astype(BF16)
        parts = [
            lax.dynamic_slice_in_dim(value, (rank ^ k) * share_rows, share_rows, 0)
            for k in range(model)
        ]
        return scatter_offsets(jnp.stack(parts), "mp")

    def spread(value):
        return gather_rows(value.astype(BF16), "mp")

    def by_owner(grad):
        return grad.reshape(data, grad.shape[0] // data, grad.shape[1])

    flat_input = layer_input[0].astype(F32)

    normed_all, _ = norm_forward(flat_input)
    hidden_1 = (normed_all * norm_gains[0]).astype(BF16)
    pre_1 = product(hidden_1, ffn1_in)
    active_1 = swish_low(pre_1)
    wide = take(layer_input[0]).astype(F32)
    normed_1, inverse_1 = norm_forward(wide[edge : edge + share_rows])
    wide = wide + 0.5 * reduce_wide(product(active_1, ffn1_out))

    width = qkv_weight.shape[2]
    heads = width // HEAD_DIM
    tables = trig_tables(frames, features)
    table = jnp.concatenate([pos_weight[0::2], pos_weight[1::2]], 0)
    table_wide = pad_lanes(table)
    bias_wide = pad_lanes(pos_bias)
    segment_row = segment.astype(F32)[None]
    normed_2, inverse_2 = norm_forward(wide[edge : edge + share_rows])
    hidden_2 = spread(normed_2 * norm_gains[1])

    units, channels_own = ffn2_out.shape[0], conv_out.shape[0]
    pack = jnp.concatenate([ffn2_in.T, ffn2_out, conv_in[0].T, conv_in[1].T, conv_out], 0)
    hidden_2, pack = lax.optimization_barrier((hidden_2, pack))
    packs = gather_offsets(pack, "mp")
    cuts = [0, units, 2 * units]
    cuts += [cuts[-1] + channels_own * k for k in (1, 2, 3)]
    ffn2_in_t, ffn2_out_all, value_t, gate_t, conv_out_all = [
        jnp.concatenate([one[low:high] for one in packs], 0) for low, high in zip(cuts, cuts[1:])
    ]
    glu_t = jnp.concatenate([value_t, gate_t], 0)
    small = jnp.concatenate([depth_kernel, bn_scale[None], bn_shift[None]], 0)
    small = jnp.concatenate(gather_offsets(small, "mp"), 1)
    taps = depth_kernel.shape[0]
    kernel_all, scale_all, shift_all = small[:taps], small[taps], small[taps + 1]

    query = pad_lanes(product(hidden_2, qkv_weight[0]))
    keys = pad_lanes(product(hidden_2, qkv_weight[1]).astype(BF16))
    values = pad_lanes(product(hidden_2, qkv_weight[2]).astype(BF16))
    mixed_wide, totals = attend(
        heads, query, keys, values, segment_row, bias_wide, table_wide, tables
    )
    mixed = mixed_wide[:, :width]
    wide = wide + reduce_wide(product(mixed, out_weight))

    normed_3, inverse_3 = norm_forward(wide)
    hidden_3 = (normed_3 * norm_gains[2]).astype(BF16)
    glu = right_product(hidden_3, glu_t)
    glu_value = glu[:, :features]
    gate_sig = jax.nn.sigmoid(glu[:, features:])
    channels = glu_value * gate_sig
    before, after = reach_of(segment, (taps - 1) // 2)
    wide_rows = (channels.shape[0], lane_groups(features)[0].stop)
    before = jnp.broadcast_to(take(before)[:, None], wide_rows)
    after = jnp.broadcast_to(take(after)[:, None], wide_rows)
    filtered = depthwise(channels, kernel_all, before, after)
    valid = (take(segment, -2) >= 0).astype(F32)[HALO:-HALO, None]
    count = jnp.sum(valid[own])
    mean = jnp.sum(valid[own] * filtered[own], 0) / jnp.maximum(count, 1.0)
    off = filtered[own] - mean
    moments = jnp.stack(
        [jnp.broadcast_to(count, mean.shape), mean, jnp.sum(valid[own] * off * off, 0)]
    )
    counts, bn_mean, bn_square = everywhere(moments, join_moments)
    bn_rstd = lax.rsqrt(bn_square / counts + NORM_EPSILON)
    centred = filtered - bn_mean
    bn_normed = centred * bn_rstd
    bn_value = bn_normed * scale_all + shift_all
    conv_act = swish_low(bn_value)
    stream = wide[HALO:-HALO] + product(conv_act, conv_out_all)

    normed_4, inverse_4 = norm_forward(stream)
    hidden_4 = (normed_4 * norm_gains[3]).astype(BF16)
    pre_4 = right_product(hidden_4, ffn2_in_t)
    active_4 = swish_low(pre_4)
    stream = stream + 0.5 * product(active_4, ffn2_out_all)
    normed_5, inverse_5 = norm_forward(stream)
    layer_output = spread(normed_5[own] * norm_gains[4])[None]

    wide_grad = take(out_cotangent[0]).astype(F32)[HALO:-HALO]
    gradient = norm_backward(wide_grad, normed_5, inverse_5, norm_gains[4])
    gain_5 = jnp.sum(wide_grad[own] * normed_5[own], 0)
    grad_out = (0.5 * gradient).astype(BF16)
    grad_pre = (right_product(grad_out, ffn2_out_all) * swish_grad(pre_4)).astype(BF16)
    grad_hidden = product(grad_pre, ffn2_in_t)
    gain_4 = jnp.sum(grad_hidden[own] * normed_4[own], 0)
    gradient = gradient + norm_backward(grad_hidden, normed_4, inverse_4, norm_gains[3])
    ffn2_in_g = left_product(hidden_4[own], grad_pre[own]).astype(BF16)
    ffn2_out_g = left_product(grad_out[own], active_4[own]).astype(BF16)

    grad_y = gradient.astype(BF16)
    conv_out_g = left_product(grad_y[own], conv_act[own]).astype(BF16)
    grad_bn = right_product(grad_y, conv_out_all) * swish_grad(bn_value)
    bn_sums = jnp.stack(
        [jnp.sum(grad_bn[own], 0), jnp.sum(grad_bn[own] * bn_normed[own], 0)]
    )
    bn_sums = everywhere(bn_sums, jnp.add)
    shift_g, scale_g = bn_sums[0], bn_sums[1]
    grad_mean = -scale_all * shift_g * bn_rstd
    grad_var = -0.5 * scale_all * scale_g * bn_rstd * bn_rstd
    grad_filtered = (
        scale_all * grad_bn * bn_rstd + valid * (grad_mean + 2.0 * grad_var * centred) / counts
    )
    grad_channels, kernel_g = depthwise_back(grad_filtered, channels, kernel_all, before, after)
    inner = slice(edge, edge + share_rows)
    sig = gate_sig[inner]
    grad_glu = jnp.concatenate(
        [grad_channels * sig, grad_channels * glu_value[inner] * sig * (1.0 - sig)], 1
    ).astype(BF16)
    grad_hidden = product(grad_glu, glu_t)
    conv_in_g = left_product(hidden_3[inner], grad_glu).astype(BF16)
    gain_3 = jnp.sum(grad_hidden * normed_3[inner], 0)
    gradient = gradient[own] + norm_backward(
        grad_hidden, normed_3[inner], inverse_3[inner], norm_gains[2]
    )

    grad_y = spread(gradient)
    grad_mixed = pad_lanes(right_product(grad_y, out_weight).astype(BF16))

    def lanes_of(grad, k, size):
        return grad[:, k * size : (k + 1) * size]

    blocks = [
        jnp.concatenate(
            [
                lanes_of(ffn2_in_g, k, units),
                lanes_of(ffn2_out_g, k, units),
                lanes_of(conv_out_g, k, channels_own),
                lanes_of(conv_in_g, k, channels_own),
                lanes_of(conv_in_g, model + k, channels_own),
            ],
            1,
        )
        for k in range(model)
    ]
    framed_g = scatter_offsets(jnp.stack(blocks), "mp").astype(BF16)
    kernel_g = jnp.stack([lanes_of(kernel_g, k, channels_own) for k in range(model)])
    kernel_g = scatter_offsets(kernel_g, "mp", F32)

    query_g, key_g, value_g, table_g, bias_g = attend_back(
        heads, query, keys, values, grad_mixed, mixed_wide, totals, segment_row, bias_wide, table_wide, tables
    )
    query_g, key_g, value_g = query_g[:, :width], key_g[:, :width], value_g[:, :width]
    qkv_cat = jnp.concatenate([query_g, key_g, value_g], 1)
    weight_cat = jnp.concatenate(list(qkv_weight), 1)
    grad_hidden = reduce(right_product(qkv_cat, weight_cat))
    gain_2 = jnp.sum(grad_hidden * normed_2, 0)
    gradient = gradient + norm_backward(grad_hidden, normed_2, inverse_2, norm_gains[1])
    half = features // 2
    table_g = table_g[:, :width]
    pos_weight_g = jnp.stack([table_g[:half], table_g[half:]], 1).reshape(features, width)
    bias_g = jnp.sum(bias_g, 1).reshape(2, -1)[:, :width]
    early = jnp.concatenate(
        [
            framed_g,
            left_product(grad_y, mixed).astype(BF16),
            left_product(hidden_2, qkv_cat).astype(BF16),
            pos_weight_g.astype(BF16),
        ],
        1,
    )
    early = scatter_chunks(by_owner(early), "dp")
    sizes = [units, units, channels_own, channels_own, channels_own] + [width] * 5
    cuts = [sum(sizes[:k]) for k in range(len(sizes) + 1)]
    ffn2_in_g, ffn2_out_g, conv_out_g, value_w_g, gate_w_g, out_weight_g, q_g, k_g, v_g, pos_g = [
        early[:, low:high] for low, high in zip(cuts, cuts[1:])
    ]

    grad_out = spread(0.5 * gradient)
    grad_pre = (right_product(grad_out, ffn1_out) * swish_grad(pre_1)).astype(BF16)
    part = right_product(grad_pre, ffn1_in)
    gain_1 = jnp.sum(part * normed_all, 0)
    grad_hidden = reduce(part)
    late = jnp.concatenate(
        [left_product(hidden_1, grad_pre).astype(BF16), left_product(grad_out, active_1).astype(BF16)], 1
    )
    late = scatter_chunks(by_owner(late), "dp")
    gradient = gradient + norm_backward(grad_hidden, normed_1, inverse_1, norm_gains[0])
    input_grad = spread(gradient)[None]

    gains = sum_small(sum_small(jnp.stack([gain_1, gain_2, gain_3, gain_4, gain_5]), "mp"), "dp")
    gain_width = features // data
    gains = lax.dynamic_slice_in_dim(gains, lax.axis_index("dp") * gain_width, gain_width, 1)
    sums = sum_small(jnp.concatenate([bias_g, kernel_g], 0), "dp")
    return (
        layer_output,
        input_grad,
        gains,
        late[:, :units],
        late[:, units:].T,
        jnp.stack([q_g, k_g, v_g]),
        pos_g,
        sums[:2],
        out_weight_g.T,
        jnp.stack([value_w_g, gate_w_g]),
        sums[2:],
        scale_g[:channels_own],
        shift_g[:channels_own],
        conv_out_g.T,
        ffn2_in_g,
        ffn2_out_g.T,
    )


def solution(mesh):
    placed = (
        P("dp", None, None),
        P("dp", None),
        P("dp", None, None),
        P(),
        P(None, "mp"),
        P("mp", None),
        P(None, None, "mp"),
        P(None, "mp"),
        P(None, "mp"),
        P("mp", None),
        P(None, None, "mp"),
        P(None, "mp"),
        P("mp"),
        P("mp"),
        P("mp", None),
        P(None, "mp"),
        P("mp", None),
    )
    return jax.shard_map(
        per_device,
        mesh=mesh,
        in_specs=placed,
        out_specs=(
            P("dp", None, None),
            P("dp", None, None),
            P(None, "dp"),
            P("dp", "mp"),
            P("mp", "dp"),
            P(None, "dp", "mp"),
            P("dp", "mp"),
            P(None, "mp"),
            P("mp", "dp"),
            P(None, "dp", "mp"),
            P(None, "mp"),
            P("mp"),
            P("mp"),
            P("mp", "dp"),
            P("dp", "mp"),
            P("mp", "dp"),
        ),
        check_vma=False,
    )
```
